32 devices in a mesh: layer: 2 (over core), row: 4 (over y, x), col: 4 (over z).
Axes of the slice: x: 2, y: 2, z: 4, core: 2. Of those that a mesh axis runs over, the one named last changes fastest.
Arguments:
- left_matrix: bfloat16 [2048, 16384], P('row', ('layer', 'col')), may hold values from -6 to 6
- right_matrix: bfloat16 [16384, 8192], P(('layer', 'row'), 'col'), may hold values from -0.046875 to 0.046875
Outputs:
- product: bfloat16 [2048, 8192], P(('row', 'layer'), 'col')
The draws below stay inside these ranges and needn't reach their ends.
All inputs are finite; a program needn't handle non-finite values.
Results may differ from the reference program's by a relative error of at most 0.001.
Values may be sent and summed in bfloat16 or wider, within the bound.
A program may use at most 128 MiB of HBM per device.

```python
import jax
import jax.numpy as jnp

K = 16384
N = 8192
M = 2048


def block_levels(stream_key, dims, split, smallest, top_value):
    level = 1.0
    for position, blocks in split:
        heights = jax.random.uniform(jax.random.fold_in(jax.random.fold_in(stream_key, 6), position), (blocks,), jnp.float32, smallest / len(split), top_value / len(split))
        level = level * jnp.repeat(jnp.exp(heights), dims[position] // blocks).reshape((-1,) + (1,) * (len(dims) - 1 - position))
    return level


def scatter_about(rng, dims, width, bound, pieces=(), kind=jnp.bfloat16):
    array = width * jax.random.normal(rng, dims, jnp.float32)
    if pieces:
        array = array * block_levels(rng, dims, pieces, -0.22, 0.18)
    return jnp.clip(array, -bound, bound).astype(kind)


def setup_inputs(seed: int = 0) -> dict:
    keys = jax.random.split(jax.random.key(seed), 3)
    left_matrix = scatter_about(keys[0], (M, K), 1.0, 6.0, ((0, 4), (1, 8)))
    right_matrix = scatter_about(keys[1], (K, N), K ** -0.5, 0.046875, ((0, 8), (1, 4)))
    return dict(left_matrix=left_matrix, right_matrix=right_matrix)


def reference(left_matrix, right_matrix):
    exact_sum = jnp.dot(left_matrix, right_matrix, preferred_element_type=jnp.float32)
    return exact_sum.astype(jnp.bfloat16)
```

```python
import functools

import jax
import jax.numpy as jnp
from jax import lax
from jax.experimental import pallas as pl
from jax.experimental.pallas import tpu as pltpu
from jax.sharding import PartitionSpec as P

MESH = pl.DeviceIdType.MESH
CHUNKS = 4
TILE = 512


def kernel(R, NC, a_hbm, b_hbm, o_hbm, zbuf, pbuf, bbuf, cbuf, xbuf, rbuf, obuf,
           la, lb, zs, zr, ps, pr, ds, dr, cs, cr):
    l = lax.axis_index("layer")
    i = lax.axis_index("row")
    z = lax.axis_index("col")
    half = NC // 2
    N = bbuf.shape[1]
    tile = min(TILE, N)

    def a_copy(c):
        return pltpu.make_async_copy(a_hbm.at[c % 2, c // 2], zbuf.at[z, c], la.at[c])

    b_copy = pltpu.make_async_copy(b_hbm, bbuf, lb)

    def z_send(d, k, c):
        sign = 1 - 2 * d
        zb = z - sign * k
        return pltpu.make_async_remote_copy(
            src_ref=zbuf.at[zb, c], dst_ref=zbuf.at[zb, c],
            send_sem=zs.at[d, k, c], recv_sem=zr.at[d, k, c],
            device_id={"col": z + sign}, device_id_type=MESH)

    def z_recv(d, k, c):
        sign = 1 - 2 * d
        zb = z - sign * k
        return pltpu.make_async_remote_copy(
            src_ref=zbuf.at[zb, c], dst_ref=zbuf.at[zb, c],
            send_sem=zs.at[d, k - 1, c], recv_sem=zr.at[d, k - 1, c],
            device_id={"col": z - sign}, device_id_type=MESH)

    def p_send(zb, c):
        r = lax.rem(i - zb + R, R)
        return pltpu.make_async_remote_copy(
            src_ref=zbuf.at[zb, c], dst_ref=pbuf.at[r - 1, c],
            send_sem=ps.at[zb, c], recv_sem=pr.at[r - 1, c],
            device_id={"row": zb}, device_id_type=MESH)

    def p_recv(r, c):
        return pltpu.make_async_remote_copy(
            src_ref=pbuf.at[r - 1, c], dst_ref=pbuf.at[r - 1, c],
            send_sem=pr.at[r - 1, c], recv_sem=pr.at[r - 1, c],
            device_id={"row": lax.rem(i + r, R)}, device_id_type=MESH)

    def d_copy(r, c, q):
        return pltpu.make_async_remote_copy(
            src_ref=cbuf.at[r, c], dst_ref=xbuf.at[r, q],
            send_sem=ds.at[r, q], recv_sem=dr.at[r, q],
            device_id={"layer": 1 - l}, device_id_type=MESH)

    def c_copy(r, c, q):
        return pltpu.make_async_remote_copy(
            src_ref=cbuf.at[r, c], dst_ref=rbuf.at[R - r - 1, q],
            send_sem=cs.at[r - 1, q], recv_sem=cr.at[R - r - 1, q],
            device_id={"row": lax.rem(i + r, R)}, device_id_type=MESH)

    def c_recv(r, q):
        return pltpu.make_async_remote_copy(
            src_ref=rbuf.at[r - 1, q], dst_ref=rbuf.at[r - 1, q],
            send_sem=cr.at[r - 1, q], recv_sem=cr.at[r - 1, q],
            device_id={"row": lax.rem(i + r, R)}, device_id_type=MESH)

    for c in range(NC):
        a_copy(c).start()
    b_copy.start()

    barrier = pltpu.get_barrier_semaphore()
    for r in range(1, R):
        pl.semaphore_signal(barrier, inc=1, device_id={"row": lax.rem(i + r, R)}, device_id_type=MESH)
    pl.semaphore_signal(barrier, inc=1, device_id={"layer": 1 - l}, device_id_type=MESH)

    @pl.when(z > 0)
    def _():
        pl.semaphore_signal(barrier, inc=1, device_id={"col": z - 1}, device_id_type=MESH)

    @pl.when(z < R - 1)
    def _():
        pl.semaphore_signal(barrier, inc=1, device_id={"col": z + 1}, device_id_type=MESH)

    pl.semaphore_wait(barrier, R + (z > 0).astype(jnp.int32) + (z < R - 1).astype(jnp.int32))

    def outward(k, c, fn_z, fn_p):
        for d in range(2):
            sign = 1 - 2 * d
            zb = z - sign * k
            nxt = z + sign

            @pl.when((zb >= 0) & (zb < R) & (nxt >= 0) & (nxt < R))
            def _():
                fn_z(z_send(d, k, c))

    @pl.loop(0, NC)
    def _(c):
        a_copy(c).wait()
        outward(0, c, lambda x: x.start(), None)

        @pl.when(z != i)
        def _():
            p_send(z, c).start()

    b_copy.wait()

    def compute(c):
        h = lax.rem(c, 2)
        q = lax.div(c, 2)
        for r in range(R):
            if r > 0:
                p_recv(r, c).wait_recv()

            @pl.loop(0, N // tile)
            def _(n):
                cols = pl.ds(pl.multiple_of(n * tile, tile), tile)
                a = zbuf[i, c] if r == 0 else pbuf[r - 1, c]
                cbuf[r, c, :, cols] = jnp.dot(a, bbuf[:, cols], preferred_element_type=jnp.float32)

            @pl.when(h != l)
            def _():
                d_copy(r, c, q).start()

        @pl.when(h == l)
        def _():
            for r in (*range(1, R), 0):
                d_copy(r, c, q).wait_recv()

                @pl.loop(0, N // tile)
                def _(n):
                    cols = pl.ds(pl.multiple_of(n * tile, tile), tile)
                    cbuf[r, c, :, cols] = cbuf[r, c, :, cols] + xbuf[r, q, :, cols]

                if r > 0:
                    c_copy(r, c, q).start()

    far = jnp.abs(z - i)
    off = jnp.maximum(far - 1, 0) * NC

    @pl.loop(0, (R - 2) * NC + 2 * NC)
    def _(s):
        @pl.when(s < (R - 1) * NC)
        def _():
            k = lax.div(s, NC) + 1
            c = lax.rem(s, NC)
            for d in range(2):
                sign = 1 - 2 * d
                zb = z - sign * k
                nxt = z + sign

                @pl.when((zb >= 0) & (zb < R))
                def _():
                    z_recv(d, k, c).wait_recv()

                    @pl.when((nxt >= 0) & (nxt < R))
                    def _():
                        z_send(d, k, c).start()

                    @pl.when(zb != i)
                    def _():
                        p_send(zb, c).start()

        u = s - off

        @pl.when((u >= 0) & (u < 2 * NC) & (lax.rem(u + 2, 2) == 1))
        def _():
            compute(lax.div(u, 2))

    for q in range(half):
        c = 2 * q + l
        for r in range(1, R):
            c_recv(r, q).wait_recv()

        @pl.loop(0, N // tile)
        def _(n):
            cols = pl.ds(pl.multiple_of(n * tile, tile), tile)
            acc = cbuf[0, c, :, cols]
            for r in range(1, R):
                acc = acc + rbuf[r - 1, q, :, cols]
            obuf[q, :, cols] = acc.astype(jnp.bfloat16)

        pltpu.make_async_copy(obuf.at[q], o_hbm.at[q], la.at[q]).start()

    @pl.loop(0, NC)
    def _(c):
        for k in range(R):
            outward(k, c, lambda x: x.wait_send(), None)
        for zb in range(R):
            @pl.when(zb != i)
            def _():
                p_send(zb, c).wait_send()

    for q in range(half):
        for r in range(R):
            d_copy(r, 2 * q + 1 - l, q).wait_send()
            if r > 0:
                c_copy(r, 2 * q + l, q).wait_send()
        pltpu.make_async_copy(obuf.at[q], o_hbm.at[q], la.at[q]).wait()


def plain(left_matrix, right_matrix):
    left_rows = lax.all_gather(left_matrix, "col", axis=1, tiled=True)
    right_joined = lax.all_gather(right_matrix, "row", axis=0, tiled=True)
    summed = lax.psum_scatter(
        jnp.dot(left_rows, right_joined, preferred_element_type=jnp.float32),
        "layer",
        scatter_dimension=0,
        tiled=True,
    )
    return summed.astype(jnp.bfloat16)


def fused(R, left_matrix, right_matrix):
    rows, K = left_matrix.shape
    N = right_matrix.shape[1]
    NC = CHUNKS
    half = NC // 2
    CH = rows // NC
    dma = pltpu.SemaphoreType.DMA
    out = pl.pallas_call(
        functools.partial(kernel, R, NC),
        out_shape=jax.ShapeDtypeStruct((half, CH, N), jnp.bfloat16),
        in_specs=[pl.BlockSpec(memory_space=pl.ANY)] * 2,
        out_specs=pl.BlockSpec(memory_space=pl.ANY),
        scratch_shapes=[
            pltpu.VMEM((R, NC, CH, K), jnp.bfloat16),
            pltpu.VMEM((R - 1, NC, CH, K), jnp.bfloat16),
            pltpu.VMEM((K, N), jnp.bfloat16),
            pltpu.VMEM((R, NC, CH, N), jnp.float32),
            pltpu.VMEM((R, half, CH, N), jnp.float32),
            pltpu.VMEM((R - 1, half, CH, N), jnp.float32),
            pltpu.VMEM((half, CH, N), jnp.bfloat16),
            dma((NC,)), dma,
            dma((2, R, NC)), dma((2, R, NC)),
            dma((R, NC)), dma((R - 1, NC)),
            dma((R, half)), dma((R, half)),
            dma((R - 1, half)), dma((R - 1, half)),
        ],
        compiler_params=pltpu.CompilerParams(
            collective_id=0, has_side_effects=True, vmem_limit_bytes=67043328),
    )(left_matrix.reshape(2, half, CH, K), right_matrix)
    return out.reshape(half * CH, N)


def solution(mesh):
    shape = mesh.shape
    fits = shape["layer"] == 2 and shape["row"] == shape["col"]
    local = functools.partial(fused, shape["row"]) if fits else plain
    in_specs = (P("row", ("layer", "col")), P(("layer", "row"), "col"))
    out_specs = P(("row", "layer"), "col")
    return jax.shard_map(local, mesh=mesh, in_specs=in_specs, out_specs=out_specs, check_vma=False)
```

```python
import functools

import jax
import jax.numpy as jnp
from jax import lax
from jax.experimental import pallas as pl
from jax.experimental.pallas import tpu as pltpu
from jax.sharding import PartitionSpec as P

MESH = pl.DeviceIdType.MESH
CHUNKS = 8
STRIPS = 8


def kernel(R, NC, NB, a_hbm, b_hbm, o_hbm, zbuf, pbuf, bown, bin_, cbuf, xbuf, rbuf, obuf,
           la, lb, zs, zr, ps, pr, bs, br, ds, dr, cs, cr, lo):
    l = lax.axis_index("layer")
    i = lax.axis_index("row")
    z = lax.axis_index("col")
    x = lax.rem(i, 2)
    y = lax.div(i, 2)
    xn = 2 * y + 1 - x
    yn = 2 * (1 - y) + x
    rows = zbuf.shape[1]
    CH = rows // NC
    half = rows // 2
    W = bown.shape[2]

    def chunk(c):
        return pl.ds(pl.multiple_of(c * CH, CH), CH)

    def a_copy(c):
        return pltpu.make_async_copy(a_hbm.at[chunk(c)], zbuf.at[z, chunk(c)], la.at[c])

    def b_copy(n):
        return pltpu.make_async_copy(b_hbm.at[:, pl.ds(n * W, W)], bown.at[n], lb.at[n])

    def remote(src, dst, send, recv, **where):
        return pltpu.make_async_remote_copy(
            src_ref=src, dst_ref=dst, send_sem=send, recv_sem=recv,
            device_id=where, device_id_type=MESH)

    def z_send(d, k, c):
        sign = 1 - 2 * d
        zb = z - sign * k
        return remote(zbuf.at[zb, chunk(c)], zbuf.at[zb, chunk(c)], zs.at[d, k, c], zr.at[d, k, c], col=z + sign)

    def z_recv(d, k, c):
        sign = 1 - 2 * d
        zb = z - sign * k
        return remote(zbuf.at[zb, chunk(c)], zbuf.at[zb, chunk(c)], zs.at[d, k - 1, c], zr.at[d, k - 1, c], col=z - sign)

    def p_send(zb, c):
        v = lax.div(zb, 2)
        return remote(zbuf.at[zb, chunk(c)], pbuf.at[v, chunk(c)], ps.at[v, c], pr.at[v, c], row=xn)

    def b_send(n):
        return remote(bown.at[n], bin_.at[n], bs.at[n], br.at[n], row=yn)

    def d_send(n):
        return remote(cbuf.at[n, 1 - l], xbuf.at[n], ds.at[n], dr.at[n], layer=1 - l)

    def c_send(n):
        return remote(cbuf.at[n, l, 1], rbuf.at[n], cs.at[n], cr.at[n], row=xn)

    for c in range(NC):
        a_copy(c).start()
    for n in range(NB):
        b_copy(n).start()

    barrier = pltpu.get_barrier_semaphore()
    pl.semaphore_signal(barrier, inc=1, device_id={"row": xn}, device_id_type=MESH)
    pl.semaphore_signal(barrier, inc=1, device_id={"row": yn}, device_id_type=MESH)
    pl.semaphore_signal(barrier, inc=1, device_id={"layer": 1 - l}, device_id_type=MESH)

    @pl.when(z > 0)
    def _():
        pl.semaphore_signal(barrier, inc=1, device_id={"col": z - 1}, device_id_type=MESH)

    @pl.when(z < R - 1)
    def _():
        pl.semaphore_signal(barrier, inc=1, device_id={"col": z + 1}, device_id_type=MESH)

    pl.semaphore_wait(barrier, 3 + (z > 0).astype(jnp.int32) + (z < R - 1).astype(jnp.int32))

    def outward(k, c, act):
        for d in range(2):
            sign = 1 - 2 * d
            zb = z - sign * k
            nxt = z + sign

            @pl.when((zb >= 0) & (zb < R) & (nxt >= 0) & (nxt < R))
            def _():
                act(z_send(d, k, c))

    @pl.loop(0, NC)
    def _(c):
        a_copy(c).wait()
        outward(0, c, lambda s: s.start())

        @pl.when(lax.rem(z, 2) != x)
        def _():
            p_send(z, c).start()

    @pl.loop(0, NB)
    def _(n):
        b_copy(n).wait()
        b_send(n).start()

    @pl.loop(0, (R - 1) * NC)
    def _(s):
        k = lax.div(s, NC) + 1
        c = lax.rem(s, NC)
        for d in range(2):
            sign = 1 - 2 * d
            zb = z - sign * k
            nxt = z + sign

            @pl.when((zb >= 0) & (zb < R))
            def _():
                z_recv(d, k, c).wait_recv()

                @pl.when((nxt >= 0) & (nxt < R))
                def _():
                    z_send(d, k, c).start()

                @pl.when(lax.rem(zb + R, 2) != x)
                def _():
                    p_send(zb, c).start()

    @pl.loop(0, NC)
    def _(c):
        for v in range(R // 2):
            remote(pbuf.at[v, chunk(c)], pbuf.at[v, chunk(c)], pr.at[v, c], pr.at[v, c], row=xn).wait_recv()

    def settle(n):
        d_send(n).wait_recv()
        cbuf[n, l, 1] = cbuf[n, l, 1] + xbuf[n, 1]
        c_send(n).start()
        cbuf[n, l, 0] = cbuf[n, l, 0] + xbuf[n, 0]

    def finish(n):
        c_send(n).wait_recv()
        obuf[n] = (cbuf[n, l, 0] + rbuf[n]).astype(jnp.bfloat16)
        pltpu.make_async_copy(obuf.at[n], o_hbm.at[:, pl.ds(n * W, W)], lo.at[n]).start()

    @pl.loop(0, NB + 1)
    def _(n):
        @pl.when(n < NB)
        def _():
            b_send(n).wait_recv()
            for s, left in ((1, pbuf), (0, zbuf)):
                near, far = (y, 1 - y) if s else (2 * y + x, 2 * (1 - y) + x)
                for h in range(2):
                    part = pl.ds(h * half, half)
                    cbuf[n, h, s] = (
                        jnp.dot(left[near, part], bown[n], preferred_element_type=jnp.float32)
                        + jnp.dot(left[far, part], bin_[n], preferred_element_type=jnp.float32))
            d_send(n).start()

        @pl.when(n > 0)
        def _():
            settle(n - 1)

    @pl.loop(0, NB)
    def _(n):
        finish(n)

    @pl.loop(0, NC)
    def _(c):
        for k in range(R):
            outward(k, c, lambda s: s.wait_send())
        for v in range(R // 2):
            p_send(2 * v + 1 - x, c).wait_send()

    @pl.loop(0, NB)
    def _(n):
        b_send(n).wait_send()
        d_send(n).wait_send()
        c_send(n).wait_send()
        pltpu.make_async_copy(obuf.at[n], o_hbm.at[:, pl.ds(n * W, W)], lo.at[n]).wait()


def plain(left_matrix, right_matrix):
    left_rows = lax.all_gather(left_matrix, "col", axis=1, tiled=True)
    right_joined = lax.all_gather(right_matrix, "row", axis=0, tiled=True)
    summed = lax.psum_scatter(
        jnp.dot(left_rows, right_joined, preferred_element_type=jnp.float32),
        "layer",
        scatter_dimension=0,
        tiled=True,
    )
    return summed.astype(jnp.bfloat16)


def fused(R, left_matrix, right_matrix):
    rows, K = left_matrix.shape
    N = right_matrix.shape[1]
    NC, NB = CHUNKS, STRIPS
    W, half = N // NB, rows // 2
    bf16, f32 = jnp.bfloat16, jnp.float32
    dma = pltpu.SemaphoreType.DMA
    return pl.pallas_call(
        functools.partial(kernel, R, NC, NB),
        out_shape=jax.ShapeDtypeStruct((half, N), bf16),
        in_specs=[pl.BlockSpec(memory_space=pl.ANY)] * 2,
        out_specs=pl.BlockSpec(memory_space=pl.ANY),
        scratch_shapes=[
            pltpu.VMEM((R, rows, K), bf16),
            pltpu.VMEM((R // 2, rows, K), bf16),
            pltpu.VMEM((NB, K, W), bf16),
            pltpu.VMEM((NB, K, W), bf16),
            pltpu.VMEM((NB, 2, 2, half, W), f32),
            pltpu.VMEM((NB, 2, half, W), f32),
            pltpu.VMEM((NB, half, W), f32),
            pltpu.VMEM((NB, half, W), bf16),
            dma((NC,)), dma((NB,)),
            dma((2, R, NC)), dma((2, R, NC)),
            dma((R // 2, NC)), dma((R // 2, NC)),
            dma((NB,)), dma((NB,)),
            dma((NB,)), dma((NB,)),
            dma((NB,)), dma((NB,)),
            dma((NB,)),
        ],
        compiler_params=pltpu.CompilerParams(
            collective_id=0, has_side_effects=True, vmem_limit_bytes=67043328),
    )(left_matrix, right_matrix)


def solution(mesh):
    shape = mesh.shape
    fits = shape["layer"] == 2 and shape["row"] == shape["col"] == 4
    local = functools.partial(fused, shape["row"]) if fits else plain
    in_specs = (P("row", ("layer", "col")), P(("layer", "row"), "col"))
    out_specs = P(("row", "layer"), "col")
    return jax.shard_map(local, mesh=mesh, in_specs=in_specs, out_specs=out_specs, check_vma=False)
```

```python
import functools

import jax
import jax.numpy as jnp
from jax import lax
from jax.experimental import pallas as pl
from jax.experimental.pallas import tpu as pltpu
from jax.sharding import PartitionSpec as P

MESH = pl.DeviceIdType.MESH
CHUNKS = 8
STRIPS = 8
EARLY = 5


def kernel(R, NC, NB, a_hbm, b_hbm, o_hbm, zbuf, pbuf, bown, bin_, cbuf, xbuf, rbuf, obuf,
           la, lb, zs, zr, ps, pr, bs, br, ds, dr, cs, cr, lo):
    l = lax.axis_index("layer")
    i = lax.axis_index("row")
    z = lax.axis_index("col")
    x = lax.rem(i, 2)
    y = lax.div(i, 2)
    xn = 2 * y + 1 - x
    yn = 2 * (1 - y) + x
    rows = zbuf.shape[1]
    CH = rows // NC
    half = rows // 2
    W = bown.shape[2]

    def chunk(c):
        return pl.ds(pl.multiple_of(c * CH, CH), CH)

    def a_copy(c):
        return pltpu.make_async_copy(a_hbm.at[chunk(c)], zbuf.at[z, chunk(c)], la.at[c])

    def b_copy(n):
        return pltpu.make_async_copy(b_hbm.at[:, pl.ds(n * W, W)], bown.at[n], lb.at[n])

    def remote(src, dst, send, recv, **where):
        return pltpu.make_async_remote_copy(
            src_ref=src, dst_ref=dst, send_sem=send, recv_sem=recv,
            device_id=where, device_id_type=MESH)

    def z_send(d, k, c):
        sign = 1 - 2 * d
        zb = z - sign * k
        return remote(zbuf.at[zb, chunk(c)], zbuf.at[zb, chunk(c)], zs.at[d, k, c], zr.at[d, k, c], col=z + sign)

    def z_recv(d, k, c):
        sign = 1 - 2 * d
        zb = z - sign * k
        return remote(zbuf.at[zb, chunk(c)], zbuf.at[zb, chunk(c)], zs.at[d, k - 1, c], zr.at[d, k - 1, c], col=z - sign)

    def p_send(zb, c):
        v = lax.div(zb, 2)
        return remote(zbuf.at[zb, chunk(c)], pbuf.at[v, chunk(c)], ps.at[v, c], pr.at[v, c], row=xn)

    def b_send(n):
        return remote(bown.at[n], bin_.at[n], bs.at[n], br.at[n], row=yn)

    def d_send(n):
        return remote(cbuf.at[n, 1 - l], xbuf.at[n], ds.at[n], dr.at[n], layer=1 - l)

    def c_send(n):
        return remote(cbuf.at[n, l, 1], rbuf.at[n], cs.at[n], cr.at[n], row=xn)

    for c in range(NC):
        a_copy(c).start()
    for n in range(NB):
        b_copy(n).start()

    barrier = pltpu.get_barrier_semaphore()
    pl.semaphore_signal(barrier, inc=1, device_id={"row": xn}, device_id_type=MESH)
    pl.semaphore_signal(barrier, inc=1, device_id={"row": yn}, device_id_type=MESH)
    pl.semaphore_signal(barrier, inc=1, device_id={"layer": 1 - l}, device_id_type=MESH)

    @pl.when(z > 0)
    def _():
        pl.semaphore_signal(barrier, inc=1, device_id={"col": z - 1}, device_id_type=MESH)

    @pl.when(z < R - 1)
    def _():
        pl.semaphore_signal(barrier, inc=1, device_id={"col": z + 1}, device_id_type=MESH)

    pl.semaphore_wait(barrier, 3 + (z > 0).astype(jnp.int32) + (z < R - 1).astype(jnp.int32))

    def outward(k, c, act):
        for d in range(2):
            sign = 1 - 2 * d
            zb = z - sign * k
            nxt = z + sign

            @pl.when((zb >= 0) & (zb < R) & (nxt >= 0) & (nxt < R))
            def _():
                act(z_send(d, k, c))

    @pl.loop(0, NC)
    def _(c):
        a_copy(c).wait()
        outward(0, c, lambda s: s.start())

        @pl.when(lax.rem(z, 2) != x)
        def _():
            p_send(z, c).start()

    @pl.loop(0, NB)
    def _(n):
        b_copy(n).wait()
        b_send(n).start()

    def z_step(s):
        k = lax.div(s, NC) + 1
        c = lax.rem(s, NC)
        for d in range(2):
            sign = 1 - 2 * d
            zb = z - sign * k
            nxt = z + sign

            @pl.when((zb >= 0) & (zb < R))
            def _():
                z_recv(d, k, c).wait_recv()

                @pl.when((nxt >= 0) & (nxt < R))
                def _():
                    z_send(d, k, c).start()

                @pl.when(lax.rem(zb + R, 2) != x)
                def _():
                    p_send(zb, c).start()

    def p_wait(c):
        for v in range(R // 2):
            remote(pbuf.at[v, chunk(c)], pbuf.at[v, chunk(c)], pr.at[v, c], pr.at[v, c], row=xn).wait_recv()

    def multiply(n, h):
        part = pl.ds(h * half, half)
        for s, left in ((1, pbuf), (0, zbuf)):
            near, far = (y, 1 - y) if s else (2 * y + x, 2 * (1 - y) + x)
            cbuf[n, h, s] = (
                jnp.dot(left[near, part], bown[n], preferred_element_type=jnp.float32)
                + jnp.dot(left[far, part], bin_[n], preferred_element_type=jnp.float32))

        @pl.when(h != l)
        def _():
            d_send(n).start()

    def settle(n):
        d_send(n).wait_recv()
        cbuf[n, l, 1] = cbuf[n, l, 1] + xbuf[n, 1]
        c_send(n).start()
        cbuf[n, l, 0] = cbuf[n, l, 0] + xbuf[n, 0]

    def finish(n):
        c_send(n).wait_recv()
        obuf[n] = (cbuf[n, l, 0] + rbuf[n]).astype(jnp.bfloat16)
        pltpu.make_async_copy(obuf.at[n], o_hbm.at[:, pl.ds(n * W, W)], lo.at[n]).start()

    def sweep(h, first):
        @pl.loop(0, EARLY + 1)
        def _(n):
            @pl.when(n < EARLY)
            def _():
                if first:
                    b_send(n).wait_recv()
                multiply(n, h)

            @pl.when((n > 0) & (l == h))
            def _():
                settle(n - 1)

    pause = (R - 2) * NC + NC // 2 + 2

    @pl.loop(0, pause)
    def _(s):
        z_step(s)

    @pl.loop(0, NC // 2)
    def _(c):
        p_wait(c)

    sweep(0, True)

    @pl.loop(pause, (R - 1) * NC)
    def _(s):
        z_step(s)

    @pl.loop(NC // 2, NC)
    def _(c):
        p_wait(c)

    sweep(1, False)

    @pl.loop(EARLY, NB)
    def _(n):
        @pl.when(n == NB - 1)
        def _():
            @pl.loop(0, NB - 2)
            def _(m):
                finish(m)

        b_send(n).wait_recv()
        multiply(n, 0)
        multiply(n, 1)
        settle(n)

    @pl.loop(NB - 2, NB)
    def _(n):
        finish(n)

    @pl.loop(0, NC)
    def _(c):
        for k in range(R):
            outward(k, c, lambda s: s.wait_send())
        for v in range(R // 2):
            p_send(2 * v + 1 - x, c).wait_send()

    @pl.loop(0, NB)
    def _(n):
        b_send(n).wait_send()
        d_send(n).wait_send()
        c_send(n).wait_send()
        pltpu.make_async_copy(obuf.at[n], o_hbm.at[:, pl.ds(n * W, W)], lo.at[n]).wait()


def plain(left_matrix, right_matrix):
    left_rows = lax.all_gather(left_matrix, "col", axis=1, tiled=True)
    right_joined = lax.all_gather(right_matrix, "row", axis=0, tiled=True)
    summed = lax.psum_scatter(
        jnp.dot(left_rows, right_joined, preferred_element_type=jnp.float32),
        "layer",
        scatter_dimension=0,
        tiled=True,
    )
    return summed.astype(jnp.bfloat16)


def fused(R, left_matrix, right_matrix):
    rows, K = left_matrix.shape
    N = right_matrix.shape[1]
    NC, NB = CHUNKS, STRIPS
    W, half = N // NB, rows // 2
    bf16, f32 = jnp.bfloat16, jnp.float32
    dma = pltpu.SemaphoreType.DMA
    return pl.pallas_call(
        functools.partial(kernel, R, NC, NB),
        out_shape=jax.ShapeDtypeStruct((half, N), bf16),
        in_specs=[pl.BlockSpec(memory_space=pl.ANY)] * 2,
        out_specs=pl.BlockSpec(memory_space=pl.ANY),
        scratch_shapes=[
            pltpu.VMEM((R, rows, K), bf16),
            pltpu.VMEM((R // 2, rows, K), bf16),
            pltpu.VMEM((NB, K, W), bf16),
            pltpu.VMEM((NB, K, W), bf16),
            pltpu.VMEM((NB, 2, 2, half, W), f32),
            pltpu.VMEM((NB, 2, half, W), f32),
            pltpu.VMEM((NB, half, W), f32),
            pltpu.VMEM((NB, half, W), bf16),
            dma((NC,)), dma((NB,)),
            dma((2, R, NC)), dma((2, R, NC)),
            dma((R // 2, NC)), dma((R // 2, NC)),
            dma((NB,)), dma((NB,)),
            dma((NB,)), dma((NB,)),
            dma((NB,)), dma((NB,)),
            dma((NB,)),
        ],
        compiler_params=pltpu.CompilerParams(
            collective_id=0, has_side_effects=True, vmem_limit_bytes=67043328),
    )(left_matrix, right_matrix)


def solution(mesh):
    shape = mesh.shape
    fits = shape["layer"] == 2 and shape["row"] == shape["col"] == 4
    local = functools.partial(fused, shape["row"]) if fits else plain
    in_specs = (P("row", ("layer", "col")), P(("layer", "row"), "col"))
    out_specs = P(("row", "layer"), "col")
    return jax.shard_map(local, mesh=mesh, in_specs=in_specs, out_specs=out_specs, check_vma=False)
```

```python
import functools

import jax
import jax.numpy as jnp
from jax import lax
from jax.experimental import pallas as pl
from jax.experimental.pallas import tpu as pltpu
from jax.sharding import PartitionSpec as P

MESH = pl.DeviceIdType.MESH
CHUNKS = 8
STRIPS = 8
LATE = 5


def kernel(R, NC, NB, a_hbm, b_hbm, o_hbm, zbuf, pbuf, bown, bin_, cbuf, xbuf, rbuf, obuf,
           la, lb, zs, zr, ps, pr, bs, br, ds, dr, cs, cr, lo):
    l = lax.axis_index("layer")
    i = lax.axis_index("row")
    z = lax.axis_index("col")
    x = lax.rem(i, 2)
    y = lax.div(i, 2)
    xn = 2 * y + 1 - x
    yn = 2 * (1 - y) + x
    rows = zbuf.shape[1]
    CH = rows // NC
    half = rows // 2
    W = bown.shape[2]

    def chunk(c):
        return pl.ds(pl.multiple_of(c * CH, CH), CH)

    def a_copy(c):
        return pltpu.make_async_copy(a_hbm.at[chunk(c)], zbuf.at[z, chunk(c)], la.at[c])

    def b_copy(n):
        return pltpu.make_async_copy(b_hbm.at[:, pl.ds(n * W, W)], bown.at[n], lb.at[n])

    def remote(src, dst, send, recv, **where):
        return pltpu.make_async_remote_copy(
            src_ref=src, dst_ref=dst, send_sem=send, recv_sem=recv,
            device_id=where, device_id_type=MESH)

    def z_send(d, k, c):
        sign = 1 - 2 * d
        zb = z - sign * k
        return remote(zbuf.at[zb, chunk(c)], zbuf.at[zb, chunk(c)], zs.at[d, k, c], zr.at[d, k, c], col=z + sign)

    def z_recv(d, k, c):
        sign = 1 - 2 * d
        zb = z - sign * k
        return remote(zbuf.at[zb, chunk(c)], zbuf.at[zb, chunk(c)], zs.at[d, k - 1, c], zr.at[d, k - 1, c], col=z - sign)

    def p_send(zb, c):
        v = lax.div(zb, 2)
        return remote(zbuf.at[zb, chunk(c)], pbuf.at[v, chunk(c)], ps.at[v, c], pr.at[v, c], row=xn)

    def b_send(n):
        return remote(bown.at[n], bin_.at[n], bs.at[n], br.at[n], row=yn)

    def d_send(n):
        return remote(cbuf.at[n, 1 - l], xbuf.at[n], ds.at[n], dr.at[n], layer=1 - l)

    def c_send(n):
        return remote(cbuf.at[n, l, 1], rbuf.at[n], cs.at[n], cr.at[n], row=xn)

    for c in range(NC):
        a_copy(c).start()
    for n in range(NB):
        b_copy(n).start()

    barrier = pltpu.get_barrier_semaphore()
    pl.semaphore_signal(barrier, inc=1, device_id={"row": xn}, device_id_type=MESH)
    pl.semaphore_signal(barrier, inc=1, device_id={"row": yn}, device_id_type=MESH)
    pl.semaphore_signal(barrier, inc=1, device_id={"layer": 1 - l}, device_id_type=MESH)

    @pl.when(z > 0)
    def _():
        pl.semaphore_signal(barrier, inc=1, device_id={"col": z - 1}, device_id_type=MESH)

    @pl.when(z < R - 1)
    def _():
        pl.semaphore_signal(barrier, inc=1, device_id={"col": z + 1}, device_id_type=MESH)

    pl.semaphore_wait(barrier, 3 + (z > 0).astype(jnp.int32) + (z < R - 1).astype(jnp.int32))

    def outward(k, c, act):
        for d in range(2):
            sign = 1 - 2 * d
            zb = z - sign * k
            nxt = z + sign

            @pl.when((zb >= 0) & (zb < R) & (nxt >= 0) & (nxt < R))
            def _():
                act(z_send(d, k, c))

    @pl.loop(0, NC)
    def _(c):
        a_copy(c).wait()
        outward(0, c, lambda s: s.start())

        @pl.when(lax.rem(z, 2) != x)
        def _():
            p_send(z, c).start()

    @pl.loop(0, NB)
    def _(n):
        b_copy(n).wait()
        b_send(n).start()

    @pl.loop(0, (R - 1) * NC)
    def _(s):
        k = lax.div(s, NC) + 1
        c = lax.rem(s, NC)
        for d in range(2):
            sign = 1 - 2 * d
            zb = z - sign * k
            nxt = z + sign

            @pl.when((zb >= 0) & (zb < R))
            def _():
                z_recv(d, k, c).wait_recv()

                @pl.when((nxt >= 0) & (nxt < R))
                def _():
                    z_send(d, k, c).start()

                @pl.when(lax.rem(zb + R, 2) != x)
                def _():
                    p_send(zb, c).start()

    @pl.loop(0, NC)
    def _(c):
        for v in range(R // 2):
            remote(pbuf.at[v, chunk(c)], pbuf.at[v, chunk(c)], pr.at[v, c], pr.at[v, c], row=xn).wait_recv()

    def settle(n):
        d_send(n).wait_recv()
        cbuf[n, l, 1] = cbuf[n, l, 1] + xbuf[n, 1]
        c_send(n).start()
        cbuf[n, l, 0] = cbuf[n, l, 0] + xbuf[n, 0]

    def finish(n):
        c_send(n).wait_recv()
        obuf[n] = (cbuf[n, l, 0] + rbuf[n]).astype(jnp.bfloat16)
        pltpu.make_async_copy(obuf.at[n], o_hbm.at[:, pl.ds(n * W, W)], lo.at[n]).start()

    def multiply(n):
        b_send(n).wait_recv()
        for s, left in ((1, pbuf), (0, zbuf)):
            near, far = (y, 1 - y) if s else (2 * y + x, 2 * (1 - y) + x)
            for h in range(2):
                part = pl.ds(h * half, half)
                cbuf[n, h, s] = (
                    jnp.dot(left[near, part], bown[n], preferred_element_type=jnp.float32)
                    + jnp.dot(left[far, part], bin_[n], preferred_element_type=jnp.float32))
        d_send(n).start()

    @pl.loop(0, NB)
    def _(n):
        multiply(n)

        @pl.when((n > 0) & (n <= LATE))
        def _():
            settle(n - 1)

        @pl.when(n >= LATE)
        def _():
            settle(n)

    @pl.loop(0, NB)
    def _(n):
        finish(n)

    @pl.loop(0, NC)
    def _(c):
        for k in range(R):
            outward(k, c, lambda s: s.wait_send())
        for v in range(R // 2):
            p_send(2 * v + 1 - x, c).wait_send()

    @pl.loop(0, NB)
    def _(n):
        b_send(n).wait_send()
        d_send(n).wait_send()
        c_send(n).wait_send()
        pltpu.make_async_copy(obuf.at[n], o_hbm.at[:, pl.ds(n * W, W)], lo.at[n]).wait()


def plain(left_matrix, right_matrix):
    left_rows = lax.all_gather(left_matrix, "col", axis=1, tiled=True)
    right_joined = lax.all_gather(right_matrix, "row", axis=0, tiled=True)
    summed = lax.psum_scatter(
        jnp.dot(left_rows, right_joined, preferred_element_type=jnp.float32),
        "layer",
        scatter_dimension=0,
        tiled=True,
    )
    return summed.astype(jnp.bfloat16)


def fused(R, left_matrix, right_matrix):
    rows, K = left_matrix.shape
    N = right_matrix.shape[1]
    NC, NB = CHUNKS, STRIPS
    W, half = N // NB, rows // 2
    bf16, f32 = jnp.bfloat16, jnp.float32
    dma = pltpu.SemaphoreType.DMA
    return pl.pallas_call(
        functools.partial(kernel, R, NC, NB),
        out_shape=jax.ShapeDtypeStruct((half, N), bf16),
        in_specs=[pl.BlockSpec(memory_space=pl.ANY)] * 2,
        out_specs=pl.BlockSpec(memory_space=pl.ANY),
        scratch_shapes=[
            pltpu.VMEM((R, rows, K), bf16),
            pltpu.VMEM((R // 2, rows, K), bf16),
            pltpu.VMEM((NB, K, W), bf16),
            pltpu.VMEM((NB, K, W), bf16),
            pltpu.VMEM((NB, 2, 2, half, W), f32),
            pltpu.VMEM((NB, 2, half, W), f32),
            pltpu.VMEM((NB, half, W), f32),
            pltpu.VMEM((NB, half, W), bf16),
            dma((NC,)), dma((NB,)),
            dma((2, R, NC)), dma((2, R, NC)),
            dma((R // 2, NC)), dma((R // 2, NC)),
            dma((NB,)), dma((NB,)),
            dma((NB,)), dma((NB,)),
            dma((NB,)), dma((NB,)),
            dma((NB,)),
        ],
        compiler_params=pltpu.CompilerParams(
            collective_id=0, has_side_effects=True, vmem_limit_bytes=67043328),
    )(left_matrix, right_matrix)


def solution(mesh):
    shape = mesh.shape
    fits = shape["layer"] == 2 and shape["row"] == shape["col"] == 4
    local = functools.partial(fused, shape["row"]) if fits else plain
    in_specs = (P("row", ("layer", "col")), P(("layer", "row"), "col"))
    out_specs = P(("row", "layer"), "col")
    return jax.shard_map(local, mesh=mesh, in_specs=in_specs, out_specs=out_specs, check_vma=False)
```
